32 devices in a mesh: batch: 8 (over z, y), mp: 4 (over x, core).
Axes of the slice: x: 2, y: 2, z: 4, core: 2. Of those that a mesh axis runs over, the one named last changes fastest.
Arguments:
- lookup_ids: int32 [64, 16384], P('batch'), may hold values from 0 to 8191
- table_feature: int32 [64], replicated, may hold values from 0 to 63, each once
- tables: bfloat16 [64, 8192, 128], P('batch'), may hold values from -6 to 6
- cross_down: bfloat16 [2, 8192, 512], P(None, 'mp'), may hold values from -0.0625 to 0.0625
- cross_up: bfloat16 [2, 512, 8192], P(None, None, 'mp'), may hold values from -0.25 to 0.25
- cross_bias: float32 [2, 8192], P(None, 'mp'), may hold values from -3 to 3
Outputs:
- crossed: bfloat16 [16384, 8192], P('batch', 'mp')
The draws below stay inside these ranges and needn't reach their ends.
Inputs may be any that keep to these rules, and one draw needn't show every extreme that they name: `table_feature`: each number appears once.
All inputs are finite; a program needn't handle non-finite values.
Results may differ from the reference program's by a relative error of at most 0.015.
Values may be sent and summed in bfloat16 or wider, within the bound.
A program may use at most 128 MiB of HBM per device.

```python
import math
import jax
import jax.numpy as jnp
import numpy as np
from jax import lax

FEATS = 64
EMB = 128
RANK = 512
ROWS = 8192
LAYERS = 2
WIDTH = 8192
BATCH = 16384
N_MP = 4


def plant(drawn, stream_key, low, top_value):
    place = [jax.random.randint(jax.random.fold_in(stream_key, axis), (), 0, length) for axis, length in enumerate(drawn.shape)]
    main_axis = drawn.shape.index(max(drawn.shape))
    neighbour = place[:main_axis] + [(place[main_axis] + 1) % drawn.shape[main_axis]] + place[main_axis + 1:]
    return drawn.at[tuple(place)].set(low).at[tuple(neighbour)].set(top_value)


def shard_levels(own_key, dims, pieces, low, high):
    factor_of = 1.0
    for axis_at, blocks in pieces:
        draws = jax.random.uniform(jax.random.fold_in(jax.random.fold_in(own_key, 6), axis_at), (blocks,), jnp.float32, low / len(pieces), high / len(pieces))
        factor_of = factor_of * jnp.repeat(jnp.exp(draws), dims[axis_at] // blocks).reshape((-1,) + (1,) * (len(dims) - 1 - axis_at))
    return factor_of


def rank_table(number_of, slope):
    weights = [(1 << 20) // math.isqrt(rank ** slope) + 1 for rank in range(1, number_of + 1)]
    width = 1 + sum(weights) // (1 << 30)
    return np.cumsum(np.array([max(1, weight // width) for weight in weights]))


def skewed_ids(stream_key, shape, amount, slope):
    grid = rank_table(amount, slope)
    lot = jax.random.randint(jax.random.fold_in(stream_key, 1), shape, 0, int(grid[amount - 1]))
    standing = jnp.searchsorted(jnp.asarray(grid, jnp.int32), lot, side="right")
    return jax.random.permutation(jax.random.fold_in(stream_key, 2), amount)[standing].astype(jnp.int32)


def centred(key, extent, width, bound, cuts=(), held_as=jnp.bfloat16):
    values = jax.random.normal(key, extent, jnp.float32) * width
    if len(cuts) > 0:
        values = shard_levels(key, extent, cuts, -0.22, 0.18) * values
    return jnp.clip(values, min=-bound, max=bound).astype(held_as)


def setup_inputs(seed: int = 0) -> dict:
    streams_of = jax.random.split(jax.random.key(seed), 7)
    lookup_ids = plant(skewed_ids(streams_of[0], (FEATS, BATCH), ROWS, 2), jax.random.fold_in(streams_of[0], 3), 0, ROWS - 1).astype(jnp.int32)
    table_feature = jax.random.permutation(streams_of[1], FEATS).astype(jnp.int32)
    tables = centred(streams_of[2], (FEATS, ROWS, EMB), 1.0, 6.0, ((0, 8),))
    cross_down = centred(streams_of[3], (LAYERS, WIDTH, RANK), WIDTH ** -0.5, 0.0625, ((1, 4),))
    cross_up = centred(streams_of[4], (LAYERS, RANK, WIDTH), RANK ** -0.5, 0.25, ((2, 4),))
    cross_bias = centred(streams_of[5], (LAYERS, WIDTH), 0.5, 3.0, ((1, 4),), jnp.float32)
    return dict(lookup_ids=lookup_ids, table_feature=table_feature, tables=tables, cross_down=cross_down, cross_up=cross_up, cross_bias=cross_bias)


def reference(lookup_ids, table_feature, tables, cross_down, cross_up, cross_bias):
    looked = jax.vmap(lambda table, index: jnp.take(table, index, axis=0))(tables, lookup_ids)
    inverse = jnp.zeros((FEATS,), jnp.int32).at[table_feature].set(jnp.arange(FEATS, dtype=jnp.int32))
    by_feature = jnp.take(looked, inverse, axis=0)
    embedded = jnp.transpose(by_feature, (1, 2, 0)).reshape(BATCH, EMB * FEATS)
    block = WIDTH // N_MP
    state = embedded
    for layer in range(LAYERS):
        low_sum = jnp.zeros((BATCH, RANK), jnp.float32)
        for piece in range(N_MP):
            term = jnp.dot(state[:, piece * block:(piece + 1) * block], cross_down[layer, piece * block:(piece + 1) * block, :], preferred_element_type=jnp.float32)
            rounded = lax.optimization_barrier(term.astype(jnp.bfloat16))
            low_sum = low_sum + rounded.astype(jnp.float32)
        low = low_sum.astype(jnp.bfloat16)
        high = jnp.dot(low, cross_up[layer], preferred_element_type=jnp.float32) + cross_bias[layer][None, :]
        state = (embedded.astype(jnp.float32) * high + state.astype(jnp.float32)).astype(jnp.bfloat16)
    return state
```

```python
import functools

import jax
import jax.numpy as jnp
from jax import lax
from jax.experimental import pallas as pl
from jax.experimental.pallas import tpu as pltpu
from jax.sharding import PartitionSpec as P

MESH = pl.DeviceIdType.MESH
GROUP = 16
LANES = 128
CORES = 2
UNROLL = 32
TILES = 4


def partner(me, mask, size):
    other = me
    bit = 1
    while bit < size:
        if mask & bit:
            other = other + bit * (1 - 2 * ((me // bit) % 2))
        bit *= 2
    return other


def kernel(
    sources,
    groups,
    feature_ref,
    bias_ref,
    ids_ref,
    tables_ref,
    down_ref,
    up_ref,
    out_ref,
    ids,
    stage,
    wide,
    rows,
    sent,
    received,
    down,
    up,
    placing,
    emb,
    mid,
    result,
    term,
    near_in,
    held,
    far_in,
    low,
    ids_sem,
    stage_sem,
    weight_sem,
    send_sem,
    recv_sem,
    reduce_send,
    reduce_recv,
    out_sem,
):
    b, m = lax.axis_index("batch"), lax.axis_index("mp")
    core = m % CORES
    side = m // CORES
    chunks, blocks, slots, emb_local, part = sent.shape
    pairs = slots // 2
    buckets = tables_ref.shape[1]
    emb_dim = tables_ref.shape[2]
    shared = emb_dim // 2
    width = down.shape[1]
    cols = placing.shape[0]
    feats = feature_ref.shape[0]
    near = (b, partner(m, 1, groups))
    far = (b, partner(m, CORES, groups))
    peers = [
        (partner(b, x, sources), side * CORES + partner(core, y, CORES), partner(core, y, CORES))
        for x in range(sources - 1, -1, -1)
        for y in range(CORES - 1, -1, -1)
        if (x, y) != (0, 0)
    ]

    ids_copy = pltpu.make_async_copy(ids_ref, ids, ids_sem)
    ids_copy.start()
    half = buckets // 2

    def stage_copies(p, h):
        span = pl.ds(h * half, half)
        return [
            pltpu.make_async_copy(
                tables_ref.at[2 * p + side, span], stage.at[h, 0], stage_sem.at[h, 0]
            ),
            pltpu.make_async_copy(
                tables_ref.at[2 * p + 1 - side, span], stage.at[h, 1], stage_sem.at[h, 1]
            ),
        ]

    for h in range(2):
        for copy in stage_copies(0, h):
            copy.start()
    weights = [
        pltpu.make_async_copy(down_ref, down, weight_sem.at[0]),
        pltpu.make_async_copy(up_ref, up, weight_sem.at[1]),
    ]

    barrier = pltpu.get_barrier_semaphore()
    greeted = [(x, y) for x, y, _ in peers] + [far]
    for peer in greeted:
        pl.semaphore_signal(barrier, inc=1, device_id=peer, device_id_type=MESH)

    def convert(p):
        for h in range(2):
            for copy in stage_copies(p, h):
                copy.wait()
            step = min(256, half)

            @pl.loop(0, half // step)
            def _(i):
                at = pl.ds(pl.multiple_of(i * step, step), step)
                to = pl.ds(pl.multiple_of(p * buckets + h * half + i * step, step), step)
                lane = lax.broadcasted_iota(jnp.int32, (step, emb_dim), 1)
                own = stage[h, 0, at, :].astype(jnp.float32)
                other = pltpu.roll(stage[h, 1, at, :].astype(jnp.float32), shared, 1)
                wide[to, :] = jnp.where(lane // shared == side, own, other)

            @pl.when(p + 1 < pairs)
            def _():
                for copy in stage_copies(p + 1, h):
                    copy.start()

    def gather(k, p):
        count = sources * part
        first = (k * pairs + p) * 2 * count
        lower = lax.broadcasted_iota(jnp.int32, (1, emb_dim), 1) < shared

        @pl.loop(0, count // UNROLL)
        def _(i):
            base = pl.multiple_of(i * UNROLL, UNROLL)
            for u in range(UNROLL):
                a = ids[first + base + u]
                c = ids[first + count + base + u]
                rows[pl.ds(base + u, 1), :] = jnp.where(
                    lower, wide[pl.ds(a, 1), :], wide[pl.ds(c, 1), :]
                )

        for d in range(sources):
            turned = rows[d * part : (d + 1) * part, :].T.astype(jnp.bfloat16)
            for s in range(2):
                for c in range(CORES):
                    at = s * shared + c * emb_local
                    sent[k, d * CORES + c, 2 * p + s] = turned[at : at + emb_local]

    def send(k):
        for x, y, c in peers:
            pltpu.make_async_remote_copy(
                src_ref=sent.at[k, x * CORES + c],
                dst_ref=received.at[k, core * sources + b],
                send_sem=send_sem.at[k],
                recv_sem=recv_sem.at[k],
                device_id=(x, y),
                device_id_type=MESH,
            ).start()
        received[k, core * sources + b] = sent[k, b * CORES + core]

    def exchanged(k):
        span = pl.ds(0, blocks - 1)
        return pltpu.make_async_remote_copy(
            src_ref=sent.at[k, span],
            dst_ref=received.at[k, span],
            send_sem=send_sem.at[k],
            recv_sem=recv_sem.at[k],
            device_id=near,
            device_id_type=MESH,
        )

    ids_copy.wait()

    @pl.loop(0, pairs)
    def _(p):
        convert(p)
        gather(0, p)

    pl.semaphore_wait(barrier, len(greeted))
    send(0)
    for copy in weights:
        copy.start()

    @pl.loop(1, chunks)
    def _(k):
        @pl.loop(0, pairs)
        def _(p):
            gather(k, p)

        send(k)

    @pl.loop(0, feats)
    def _(s):
        column = lax.broadcasted_iota(jnp.int32, (GROUP, cols), 1)
        e = lax.broadcasted_iota(jnp.int32, (GROUP, cols), 0)
        placing[pl.ds(pl.multiple_of(s * GROUP, GROUP), GROUP), :] = jnp.where(
            column == feature_ref[s] + feats * e, 1.0, 0.0
        ).astype(jnp.bfloat16)

    for copy in weights:
        copy.wait()

    size = 2 * part
    mine = pl.ds(pl.multiple_of(core * part, part), part)
    theirs = pl.ds(pl.multiple_of((1 - core) * part, part), part)

    def remote(src, dst, kind, layer, slot, peer):
        return pltpu.make_async_remote_copy(
            src_ref=src,
            dst_ref=dst,
            send_sem=reduce_send.at[kind, layer, slot],
            recv_sem=reduce_recv.at[kind, layer, slot],
            device_id=peer,
            device_id_type=MESH,
        )

    def to_near(layer, slot):
        return remote(
            term.at[layer, slot, theirs], near_in.at[layer, slot], 0, layer, slot, near
        )

    def to_far(layer, slot):
        return remote(held.at[layer, slot], far_in.at[layer, slot], 1, layer, slot, far)

    def back(layer, slot):
        place = low.at[layer, slot, mine]
        return remote(place, place, 2, layer, slot, near)

    def reduce_middle(layer, slot):
        to_near(layer, slot).wait_recv()
        held[layer, slot] = (
            term[layer, slot, mine].astype(jnp.float32) + near_in[layer, slot].astype(jnp.float32)
        ).astype(jnp.bfloat16)
        to_far(layer, slot).start()

    def reduce_last(layer, slot):
        to_far(layer, slot).wait_recv()
        low[layer, slot, mine] = (
            held[layer, slot].astype(jnp.float32) + far_in[layer, slot].astype(jnp.float32)
        ).astype(jnp.bfloat16)
        back(layer, slot).start()

    def reduce_done(layer, slot):
        back(layer, slot).wait_recv()
        to_near(layer, slot).wait_send()
        to_far(layer, slot).wait_send()
        back(layer, slot).wait_send()

    def enter(k, slot):
        exchanged(k).wait_recv()
        for j in range(emb_local // GROUP):
            sides = [
                received[
                    k, h * sources : (h + 1) * sources, :, j * GROUP : (j + 1) * GROUP
                ].reshape(cols, part)
                for h in range(2)
            ]
            emb[slot, :, j * cols : (j + 1) * cols] = lax.dot_general(
                jnp.concatenate(sides, axis=1),
                placing[...],
                (((0,), (0,)), ((), ())),
                preferred_element_type=jnp.float32,
            ).astype(jnp.bfloat16)
        term[0, slot] = jnp.dot(
            emb[slot], down[0], preferred_element_type=jnp.float32
        ).astype(jnp.bfloat16)
        to_near(0, slot).start()

    tile = width // TILES

    def cross(layer, slot, state, new):
        for n in range(TILES):
            at = slice(n * tile, (n + 1) * tile)
            high = (
                jnp.dot(low[layer, slot], up[layer, :, at], preferred_element_type=jnp.float32)
                + bias_ref[layer, at][None, :]
            )
            new[slot, :, at] = (
                emb[slot, :, at].astype(jnp.float32) * high
                + state[slot, :, at].astype(jnp.float32)
            ).astype(jnp.bfloat16)

    def out_copies(k, slot):
        return [
            pltpu.make_async_copy(
                result.at[slot, pl.ds(h * part, part)],
                out_ref.at[pl.ds(pl.multiple_of((h * chunks + k) * part, part), part)],
                out_sem.at[slot, h],
            )
            for h in range(2)
        ]

    @pl.loop(0, chunks + 1)
    def _(k):
        slot = k % 2
        last = (k + 1) % 2

        @pl.when(k < chunks)
        def _():
            enter(k, slot)

        @pl.when(k > 0)
        def _():
            reduce_middle(1, last)

        @pl.when(k < chunks)
        def _():
            reduce_middle(0, slot)

        @pl.when(k > 0)
        def _():
            reduce_last(1, last)

        @pl.when(k < chunks)
        def _():
            reduce_last(0, slot)

        @pl.when(k > 0)
        def _():
            reduce_done(1, last)

            @pl.when(k > 2)
            def _():
                for copy in out_copies(k - 3, last):
                    copy.wait()

            cross(1, last, mid, result)
            for copy in out_copies(k - 1, last):
                copy.start()

        @pl.when(k < chunks)
        def _():
            reduce_done(0, slot)
            cross(0, slot, emb, mid)
            term[1, slot] = jnp.dot(
                mid[slot], down[1], preferred_element_type=jnp.float32
            ).astype(jnp.bfloat16)
            to_near(1, slot).start()

    for k in range(max(chunks - 2, 0), chunks):
        for copy in out_copies(k, k % 2):
            copy.wait()

    @pl.loop(0, chunks)
    def _(k):
        exchanged(k).wait_send()


def pipeline(table_feature, bias, ids, tables, cross_down, cross_up, chunks, sources, groups):
    slots, buckets, emb_dim = tables.shape
    layers, width, rank = cross_down.shape
    feats = table_feature.shape[0]
    emb_local = emb_dim // groups
    part = LANES
    size = 2 * part
    pairs = slots // 2
    blocks = CORES * sources
    dma = pltpu.SemaphoreType.DMA
    bf16, f32 = jnp.bfloat16, jnp.float32
    return pl.pallas_call(
        functools.partial(kernel, sources, groups),
        out_shape=jax.ShapeDtypeStruct((chunks * size, width), bf16),
        in_specs=[
            pl.BlockSpec(memory_space=pltpu.SMEM),
            pl.BlockSpec(memory_space=pltpu.VMEM),
        ]
        + [pl.BlockSpec(memory_space=pl.ANY)] * 4,
        out_specs=pl.BlockSpec(memory_space=pl.ANY),
        scratch_shapes=[
            pltpu.SMEM(ids.shape, jnp.int32),
            pltpu.VMEM((2, 2, buckets // 2, emb_dim), bf16),
            pltpu.VMEM((pairs * buckets, emb_dim), f32),
            pltpu.VMEM((sources * part, emb_dim), f32),
            pltpu.VMEM((chunks, blocks, slots, emb_local, part), bf16),
            pltpu.VMEM((chunks, blocks, slots, emb_local, part), bf16),
            pltpu.VMEM((layers, width, rank), bf16),
            pltpu.VMEM((layers, rank, width), bf16),
            pltpu.VMEM((feats * GROUP, feats * GROUP), bf16),
            pltpu.VMEM((2, size, width), bf16),
            pltpu.VMEM((2, size, width), bf16),
            pltpu.VMEM((2, size, width), bf16),
            pltpu.VMEM((layers, 2, size, rank), bf16),
            pltpu.VMEM((layers, 2, part, rank), bf16),
            pltpu.VMEM((layers, 2, part, rank), bf16),
            pltpu.VMEM((layers, 2, part, rank), bf16),
            pltpu.VMEM((layers, 2, size, rank), bf16),
            dma,
            dma((2, 2)),
            dma((2,)),
            dma((chunks,)),
            dma((chunks,)),
            dma((3, layers, 2)),
            dma((3, layers, 2)),
            dma((2, 2)),
        ],
        compiler_params=pltpu.CompilerParams(
            collective_id=0, has_side_effects=True, vmem_limit_bytes=67_043_328
        ),
        name="pipeline",
    )(table_feature, bias, ids, tables, cross_down, cross_up)


def per_device(lookup_ids, table_feature, tables, cross_down, cross_up, cross_bias):
    slots, buckets, _ = tables.shape
    sources = lax.axis_size("batch")
    groups = lax.axis_size("mp")
    examples = lookup_ids.shape[1] // sources
    mine = examples // CORES
    chunks = mine // LANES
    start = (lax.axis_index("mp") % CORES) * mine
    wanted = lax.dynamic_slice_in_dim(
        lookup_ids.reshape(slots, sources, examples), start, mine, 2
    ).reshape(slots // 2, 2, sources, chunks, LANES)
    wanted = wanted + buckets * jnp.arange(slots // 2, dtype=jnp.int32)[:, None, None, None, None]
    ids = wanted.transpose(3, 0, 1, 2, 4).reshape(-1)
    return pipeline(
        table_feature, cross_bias, ids, tables, cross_down, cross_up, chunks, sources, groups
    )


def solution(mesh):
    return jax.shard_map(
        per_device,
        mesh=mesh,
        in_specs=(
            P("batch", None),
            P(),
            P("batch", None, None),
            P(None, "mp", None),
            P(None, None, "mp"),
            P(None, "mp"),
        ),
        out_specs=P("batch", "mp"),
        check_vma=False,
    )
```

```python
import functools

import jax
import jax.numpy as jnp
from jax import lax
from jax.experimental import pallas as pl
from jax.experimental.pallas import tpu as pltpu
from jax.sharding import PartitionSpec as P

MESH = pl.DeviceIdType.MESH
GROUP = 16
LANES = 128
CORES = 2
TILES = 4
AHEAD = 3
PHASES = 4
STEPS = 4
PIECES = 16
LIMIT = 67_043_328


def partner(me, mask, size):
    other = me
    bit = 1
    while bit < size:
        if mask & bit:
            other = other + bit * (1 - 2 * ((me // bit) % 2))
        bit *= 2
    return other


def kernel(
    sources,
    groups,
    feature_ref,
    bias_ref,
    ids_ref,
    tables_ref,
    down_ref,
    up_ref,
    out_ref,
    ids,
    stage,
    wide,
    rows,
    sent,
    received,
    down,
    up,
    placing,
    emb,
    mid,
    result,
    term,
    near_in,
    held,
    far_in,
    low,
    ids_sem,
    stage_sem,
    weight_sem,
    send_sem,
    recv_sem,
    reduce_send,
    reduce_recv,
    out_sem,
):
    b, m = lax.axis_index("batch"), lax.axis_index("mp")
    core = m % CORES
    side = m // CORES
    chunks, blocks, slots, emb_local, part = received.shape
    ring = sent.shape[0]
    pairs = slots // 2
    buckets = tables_ref.shape[1]
    emb_dim = tables_ref.shape[2]
    shared = emb_dim // 2
    width = down.shape[1]
    cols = placing.shape[0]
    feats = feature_ref.shape[0]
    near = (b, partner(m, 1, groups))
    far = (b, partner(m, CORES, groups))
    peers = [
        (partner(b, x, sources), side * CORES + partner(core, y, CORES), partner(core, y, CORES))
        for x in range(sources - 1, -1, -1)
        for y in range(CORES - 1, -1, -1)
        if (x, y) != (0, 0)
    ]

    def ids_copy(k, d):
        start = d * (2 * chunks * part) + (core * chunks + k) * part
        return pltpu.make_async_copy(
            ids_ref.at[:, pl.ds(pl.multiple_of(start, part), part)], ids.at[k, d], ids_sem.at[k]
        )

    span = buckets // STEPS

    def stage_copy(i):
        return pltpu.make_async_copy(
            tables_ref.at[pl.ds(2 * (i // STEPS), 2), pl.ds(i % STEPS * span, span)],
            stage.at[i % 2],
            stage_sem.at[i % 2],
        )

    stage_copy(0).start()
    for d in range(sources):
        ids_copy(0, d).start()
    stage_copy(1).start()

    barrier = pltpu.get_barrier_semaphore()
    greeted = [(x, y) for x, y, _ in peers] + [far]
    for peer in greeted:
        pl.semaphore_signal(barrier, inc=1, device_id=peer, device_id_type=MESH)

    @pl.loop(1, chunks)
    def _(k):
        for d in range(sources):
            ids_copy(k, d).start()

    weights = [
        pltpu.make_async_copy(down_ref, down, weight_sem.at[0]),
        pltpu.make_async_copy(up_ref, up, weight_sem.at[1]),
    ]

    def convert(p):
        for i in range(p * STEPS, (p + 1) * STEPS):
            stage_copy(i).wait()
            step = min(1024, span)

            @pl.loop(0, span // step)
            def _(t, i=i):
                at = pl.ds(pl.multiple_of(t * step, step), step)
                to = pl.ds(pl.multiple_of(i * span + t * step, step), step)
                lane = lax.broadcasted_iota(jnp.int32, (step, emb_dim), 1)
                own = stage[i % 2, side, at, :].astype(jnp.float32)
                other = pltpu.roll(stage[i % 2, 1 - side, at, :].astype(jnp.float32), shared, 1)
                wide[to, :] = jnp.where(lane // shared == side, own, other)

            if i + 2 < pairs * STEPS:
                stage_copy(i + 2).start()

    def gather(k, p):
        lower = lax.broadcasted_iota(jnp.int32, (1, emb_dim), 1) < shared
        table = wide.at[pl.ds(p * buckets, buckets)]

        @pl.loop(0, sources)
        def _(d):
            base = pl.multiple_of(d * part, part)
            for u in range(part):
                one = table[pl.ds(ids[k, d, 2 * p, u], 1), :]
                two = table[pl.ds(ids[k, d, 2 * p + 1, u], 1), :]
                rows[pl.ds(base + u, 1), :] = jnp.where(lower, one, two)

        for d in range(sources):
            turned = rows[d * part : (d + 1) * part, :].T.astype(jnp.bfloat16)
            for s in range(2):
                for c in range(CORES):
                    at = s * shared + c * emb_local
                    sent[k % ring, d * CORES + c, 2 * p + s] = turned[at : at + emb_local]

    def send(k, span):
        for x, y, c in peers:
            pltpu.make_async_remote_copy(
                src_ref=sent.at[k % ring, x * CORES + c, span],
                dst_ref=received.at[k, core * sources + b, span],
                send_sem=send_sem.at[k],
                recv_sem=recv_sem.at[k],
                device_id=(x, y),
                device_id_type=MESH,
            ).start()

    def keep(k):
        received[k, core * sources + b] = sent[k % ring, b * CORES + core]

    def exchanged(k):
        span = pl.ds(0, blocks - 1)
        return pltpu.make_async_remote_copy(
            src_ref=sent.at[k % ring, span],
            dst_ref=received.at[k, span],
            send_sem=send_sem.at[k],
            recv_sem=recv_sem.at[k],
            device_id=near,
            device_id_type=MESH,
        )

    def ids_wait(k):
        pltpu.make_async_copy(ids.at[k], ids.at[k], ids_sem.at[k]).wait()

    ids_wait(0)
    for p in range(pairs):
        convert(p)
        gather(0, p)
        if p == 0:
            pl.semaphore_wait(barrier, len(greeted))
        send(0, pl.ds(2 * p, 2))
    keep(0)
    for copy in weights:
        copy.start()

    @pl.loop(1, min(AHEAD, chunks))
    def _(k):
        ids_wait(k)
        for p in range(pairs):
            gather(k, p)
        send(k, pl.ds(0, slots))
        keep(k)

    @pl.loop(0, feats)
    def _(s):
        column = lax.broadcasted_iota(jnp.int32, (GROUP, cols), 1)
        e = lax.broadcasted_iota(jnp.int32, (GROUP, cols), 0)
        placing[pl.ds(pl.multiple_of(s * GROUP, GROUP), GROUP), :] = jnp.where(
            column == feature_ref[s] + feats * e, 1.0, 0.0
        ).astype(jnp.bfloat16)

    for copy in weights:
        copy.wait()

    share = part // 2
    mine = pl.ds(pl.multiple_of(core * share, share), share)
    theirs = pl.ds(pl.multiple_of((1 - core) * share, share), share)

    def remote(src, dst, kind, layer, h, peer):
        return pltpu.make_async_remote_copy(
            src_ref=src,
            dst_ref=dst,
            send_sem=reduce_send.at[kind, layer, h],
            recv_sem=reduce_recv.at[kind, layer, h],
            device_id=peer,
            device_id_type=MESH,
        )

    def to_near(layer, h):
        return remote(term.at[layer, h, theirs], near_in.at[layer, h], 0, layer, h, near)

    def to_far(layer, h):
        return remote(held.at[layer, h], far_in.at[layer, h], 1, layer, h, far)

    def back(layer, h):
        place = low.at[layer, h, mine]
        return remote(place, place, 2, layer, h, near)

    def reduce_middle(layer, h):
        to_near(layer, h).wait_recv()
        held[layer, h] = (
            term[layer, h, mine].astype(jnp.float32) + near_in[layer, h].astype(jnp.float32)
        ).astype(jnp.bfloat16)
        to_far(layer, h).start()

    def reduce_last(layer, h):
        to_far(layer, h).wait_recv()
        low[layer, h, mine] = (
            held[layer, h].astype(jnp.float32) + far_in[layer, h].astype(jnp.float32)
        ).astype(jnp.bfloat16)
        back(layer, h).start()

    def reduce_done(layer, h):
        back(layer, h).wait_recv()
        to_near(layer, h).wait_send()
        to_far(layer, h).wait_send()
        back(layer, h).wait_send()

    def project(layer, h, state):
        term[layer, h] = jnp.dot(
            state[h], down[layer], preferred_element_type=jnp.float32
        ).astype(jnp.bfloat16)
        to_near(layer, h).start()

    def enter(k, h):
        for j in range(emb_local // GROUP):
            x = received[k, h * sources : (h + 1) * sources, :, j * GROUP : (j + 1) * GROUP]
            emb[h, :, j * cols : (j + 1) * cols] = lax.dot_general(
                x.reshape(cols, part),
                placing[...],
                (((0,), (0,)), ((), ())),
                preferred_element_type=jnp.float32,
            ).astype(jnp.bfloat16)
        project(0, h, emb)

    tile = width // TILES

    def cross(layer, h, state, store):
        for n in range(TILES):
            at = slice(n * tile, (n + 1) * tile)
            high = (
                jnp.dot(low[layer, h], up[layer, :, at], preferred_element_type=jnp.float32)
                + bias_ref[layer, at][None, :]
            )
            store(
                at,
                (
                    emb[h, :, at].astype(jnp.float32) * high + state[h, :, at].astype(jnp.float32)
                ).astype(jnp.bfloat16),
            )

    def out_copy(k, h):
        span = pl.ds(pl.multiple_of((h * chunks + k) * part, part), part)
        return pltpu.make_async_copy(result.at[h], out_ref.at[span], out_sem.at[h])

    @pl.loop(0, chunks)
    def _(k):
        ahead = k + AHEAD
        more = ahead < chunks

        def look_up(phase):
            for p in range(pairs):
                if p * PHASES // pairs == phase:

                    @pl.when(more)
                    def _(p=p):
                        gather(ahead, p)

        @pl.when(more)
        def _():
            ids_wait(ahead)

            @pl.when(ahead >= ring)
            def _():
                exchanged(ahead - ring).wait_send()

        exchanged(k).wait_recv()
        for h in range(2):
            enter(k, h)
        look_up(0)
        for h in range(2):
            reduce_middle(0, h)
        look_up(1)
        for h in range(2):
            reduce_last(0, h)
        for h in range(2):
            reduce_done(0, h)

            def to_mid(at, value, h=h):
                mid[h, :, at] = value

            cross(0, h, emb, to_mid)
            project(1, h, mid)
        look_up(2)
        for h in range(2):
            reduce_middle(1, h)
        look_up(3)

        @pl.when(more)
        def _():
            send(ahead, pl.ds(0, slots))
            keep(ahead)

        for h in range(2):
            reduce_last(1, h)
        for h in range(2):
            reduce_done(1, h)

            @pl.when(k > 0)
            def _(h=h):
                out_copy(k - 1, h).wait()

            def to_out(at, value, h=h):
                result[h, :, at] = value

            cross(1, h, mid, to_out)
            out_copy(k, h).start()

    for h in range(2):
        out_copy(chunks - 1, h).wait()

    @pl.loop(max(chunks - ring, 0), chunks)
    def _(k):
        exchanged(k).wait_send()


def pipeline(table_feature, bias, ids, tables, cross_down, cross_up, sources, groups):
    slots, buckets, emb_dim = tables.shape
    layers, width, rank = cross_down.shape
    feats = table_feature.shape[0]
    emb_local = emb_dim // groups
    part = LANES
    share = part // 2
    chunks = ids.shape[1] // sources // (2 * part)
    pairs = slots // 2
    blocks = CORES * sources
    dma = pltpu.SemaphoreType.DMA
    bf16, f32 = jnp.bfloat16, jnp.float32
    return pl.pallas_call(
        functools.partial(kernel, sources, groups),
        out_shape=jax.ShapeDtypeStruct((chunks * 2 * part, width), bf16),
        in_specs=[
            pl.BlockSpec(memory_space=pltpu.SMEM),
            pl.BlockSpec(memory_space=pltpu.VMEM),
        ]
        + [pl.BlockSpec(memory_space=pl.ANY)] * 4,
        out_specs=pl.BlockSpec(memory_space=pl.ANY),
        scratch_shapes=[
            pltpu.SMEM((chunks, sources, slots, part), jnp.int32),
            pltpu.VMEM((2, 2, buckets // STEPS, emb_dim), bf16),
            pltpu.VMEM((pairs * buckets, emb_dim), f32),
            pltpu.VMEM((sources * part, emb_dim), f32),
            pltpu.VMEM((min(AHEAD + 1, chunks), blocks, slots, emb_local, part), bf16),
            pltpu.VMEM((chunks, blocks, slots, emb_local, part), bf16),
            pltpu.VMEM((layers, width, rank), bf16),
            pltpu.VMEM((layers, rank, width), bf16),
            pltpu.VMEM((feats * GROUP, feats * GROUP), bf16),
            pltpu.VMEM((2, part, width), bf16),
            pltpu.VMEM((2, part, width), bf16),
            pltpu.VMEM((2, part, width), bf16),
            pltpu.VMEM((layers, 2, part, rank), bf16),
            pltpu.VMEM((layers, 2, share, rank), bf16),
            pltpu.VMEM((layers, 2, share, rank), bf16),
            pltpu.VMEM((layers, 2, share, rank), bf16),
            pltpu.VMEM((layers, 2, part, rank), bf16),
            dma((chunks,)),
            dma((2,)),
            dma((2,)),
            dma((chunks,)),
            dma((chunks,)),
            dma((3, layers, 2)),
            dma((3, layers, 2)),
            dma((2,)),
        ],
        compiler_params=pltpu.CompilerParams(
            collective_id=0, has_side_effects=True, vmem_limit_bytes=LIMIT
        ),
        name="pipeline",
    )(table_feature, bias, ids, tables, cross_down, cross_up)


def finish_kernel(x_ref, out_ref, held, read_sem, write_sem):
    pieces, rows = held.shape[:2]

    def read(i):
        return pltpu.make_async_copy(x_ref.at[pl.ds(i * rows, rows)], held.at[i], read_sem.at[i])

    def write(i):
        return pltpu.make_async_copy(held.at[i], out_ref.at[pl.ds(i * rows, rows)], write_sem.at[i])

    for i in range(pieces):
        read(i).start()
    for i in range(pieces):
        read(i).wait()
        write(i).start()
    for i in range(pieces):
        write(i).wait()


def finish(x):
    rows, width = x.shape
    dma = pltpu.SemaphoreType.DMA
    return pl.pallas_call(
        finish_kernel,
        out_shape=jax.ShapeDtypeStruct(x.shape, x.dtype),
        in_specs=[pl.BlockSpec(memory_space=pl.ANY)],
        out_specs=pl.BlockSpec(memory_space=pl.ANY),
        scratch_shapes=[
            pltpu.VMEM((PIECES, rows // PIECES, width), x.dtype),
            dma((PIECES,)),
            dma((PIECES,)),
        ],
        compiler_params=pltpu.CompilerParams(vmem_limit_bytes=LIMIT),
        name="finish",
    )(x)


def per_device(lookup_ids, table_feature, tables, cross_down, cross_up, cross_bias):
    sources = lax.axis_size("batch")
    groups = lax.axis_size("mp")
    return finish(
        pipeline(
            table_feature, cross_bias, lookup_ids, tables, cross_down, cross_up, sources, groups
        )
    )


def solution(mesh):
    return jax.shard_map(
        per_device,
        mesh=mesh,
        in_specs=(
            P("batch", None),
            P(),
            P("batch", None, None),
            P(None, "mp", None),
            P(None, None, "mp"),
            P(None, "mp"),
        ),
        out_specs=P("batch", "mp"),
        check_vma=False,
    )
```

```python
import functools

import jax
import jax.numpy as jnp
from jax import lax
from jax.experimental import pallas as pl
from jax.experimental.pallas import tpu as pltpu
from jax.sharding import PartitionSpec as P

MESH = pl.DeviceIdType.MESH
GROUP = 16
LANES = 128
CORES = 2
TILES = 4
AHEAD = 3
PHASES = 4
STEPS = 4
PIECES = 8
LIMIT = 67_043_328


def partner(me, mask, size):
    other = me
    bit = 1
    while bit < size:
        if mask & bit:
            other = other + bit * (1 - 2 * ((me // bit) % 2))
        bit *= 2
    return other


def kernel(
    sources,
    groups,
    feature_ref,
    bias_ref,
    ids_ref,
    tables_ref,
    down_ref,
    up_ref,
    out_ref,
    ids,
    stage,
    wide,
    rows,
    sent,
    received,
    down,
    up,
    placing,
    emb,
    mid,
    result,
    term,
    near_in,
    held,
    far_in,
    low,
    ids_sem,
    stage_sem,
    weight_sem,
    send_sem,
    recv_sem,
    reduce_send,
    reduce_recv,
    out_sem,
):
    b, m = lax.axis_index("batch"), lax.axis_index("mp")
    core = m % CORES
    side = m // CORES
    chunks, blocks, slots, emb_local, part = received.shape
    ring = sent.shape[0]
    pairs = slots // 2
    buckets = tables_ref.shape[1]
    emb_dim = tables_ref.shape[2]
    shared = emb_dim // 2
    width = down.shape[1]
    cols = placing.shape[0]
    feats = feature_ref.shape[0]
    near = (b, partner(m, 1, groups))
    far = (b, partner(m, CORES, groups))
    peers = [
        (partner(b, x, sources), side * CORES + partner(core, y, CORES), partner(core, y, CORES))
        for x in range(sources - 1, -1, -1)
        for y in range(CORES - 1, -1, -1)
        if (x, y) != (0, 0)
    ]

    def ids_copy(k, d):
        start = d * (2 * chunks * part) + (core * chunks + k) * part
        return pltpu.make_async_copy(
            ids_ref.at[:, pl.ds(pl.multiple_of(start, part), part)], ids.at[k, d], ids_sem.at[k]
        )

    span = buckets // STEPS

    def stage_copy(i):
        return pltpu.make_async_copy(
            tables_ref.at[pl.ds(2 * (i // STEPS), 2), pl.ds(i % STEPS * span, span)],
            stage.at[i % 2],
            stage_sem.at[i % 2],
        )

    stage_copy(0).start()
    for d in range(sources):
        ids_copy(0, d).start()
    stage_copy(1).start()

    barrier = pltpu.get_barrier_semaphore()
    greeted = [(x, y) for x, y, _ in peers] + [far]
    for peer in greeted:
        pl.semaphore_signal(barrier, inc=1, device_id=peer, device_id_type=MESH)

    @pl.loop(1, chunks)
    def _(k):
        for d in range(sources):
            ids_copy(k, d).start()

    weights = [
        pltpu.make_async_copy(down_ref, down, weight_sem.at[0]),
        pltpu.make_async_copy(up_ref, up, weight_sem.at[1]),
    ]

    def convert(p):
        for i in range(p * STEPS, (p + 1) * STEPS):
            stage_copy(i).wait()
            step = min(1024, span)

            @pl.loop(0, span // step)
            def _(t, i=i):
                at = pl.ds(pl.multiple_of(t * step, step), step)
                to = pl.ds(pl.multiple_of(i * span + t * step, step), step)
                lane = lax.broadcasted_iota(jnp.int32, (step, emb_dim), 1)
                own = stage[i % 2, side, at, :].astype(jnp.float32)
                other = pltpu.roll(stage[i % 2, 1 - side, at, :].astype(jnp.float32), shared, 1)
                wide[to, :] = jnp.where(lane // shared == side, own, other)

            if i + 2 < pairs * STEPS:
                stage_copy(i + 2).start()

    def gather(k, p):
        lower = lax.broadcasted_iota(jnp.int32, (1, emb_dim), 1) < shared
        table = wide.at[pl.ds(p * buckets, buckets)]

        @pl.loop(0, sources)
        def _(d):
            base = pl.multiple_of(d * part, part)
            for u in range(part):
                one = table[pl.ds(ids[k, d, 2 * p, u], 1), :]
                two = table[pl.ds(ids[k, d, 2 * p + 1, u], 1), :]
                rows[pl.ds(base + u, 1), :] = jnp.where(lower, one, two)

        for d in range(sources):
            turned = rows[d * part : (d + 1) * part, :].T.astype(jnp.bfloat16)
            for s in range(2):
                for c in range(CORES):
                    at = s * shared + c * emb_local
                    sent[k % ring, d * CORES + c, 2 * p + s] = turned[at : at + emb_local]

    def send(k, span):
        for x, y, c in peers:
            pltpu.make_async_remote_copy(
                src_ref=sent.at[k % ring, x * CORES + c, span],
                dst_ref=received.at[k, core * sources + b, span],
                send_sem=send_sem.at[k],
                recv_sem=recv_sem.at[k],
                device_id=(x, y),
                device_id_type=MESH,
            ).start()

    def keep(k):
        received[k, core * sources + b] = sent[k % ring, b * CORES + core]

    def exchanged(k):
        span = pl.ds(0, blocks - 1)
        return pltpu.make_async_remote_copy(
            src_ref=sent.at[k % ring, span],
            dst_ref=received.at[k, span],
            send_sem=send_sem.at[k],
            recv_sem=recv_sem.at[k],
            device_id=near,
            device_id_type=MESH,
        )

    def ids_wait(k):
        pltpu.make_async_copy(ids.at[k], ids.at[k], ids_sem.at[k]).wait()

    ids_wait(0)
    for p in range(pairs):
        convert(p)
        gather(0, p)
        if p == 0:
            pl.semaphore_wait(barrier, len(greeted))
        send(0, pl.ds(2 * p, 2))
    keep(0)
    for copy in weights:
        copy.start()

    @pl.loop(1, min(AHEAD, chunks))
    def _(k):
        ids_wait(k)
        for p in range(pairs):
            gather(k, p)
        send(k, pl.ds(0, slots))
        keep(k)

    @pl.loop(0, feats)
    def _(s):
        column = lax.broadcasted_iota(jnp.int32, (GROUP, cols), 1)
        e = lax.broadcasted_iota(jnp.int32, (GROUP, cols), 0)
        placing[pl.ds(pl.multiple_of(s * GROUP, GROUP), GROUP), :] = jnp.where(
            column == feature_ref[s] + feats * e, 1.0, 0.0
        ).astype(jnp.bfloat16)

    for copy in weights:
        copy.wait()

    share = part // 2
    mine = pl.ds(pl.multiple_of(core * share, share), share)
    theirs = pl.ds(pl.multiple_of((1 - core) * share, share), share)

    def remote(src, dst, kind, layer, h, peer):
        return pltpu.make_async_remote_copy(
            src_ref=src,
            dst_ref=dst,
            send_sem=reduce_send.at[kind, layer, h],
            recv_sem=reduce_recv.at[kind, layer, h],
            device_id=peer,
            device_id_type=MESH,
        )

    def to_near(layer, h):
        return remote(term.at[layer, h, theirs], near_in.at[layer, h], 0, layer, h, near)

    def turn(layer, k):
        return 2 * layer + k % 2

    def to_far(layer, h, k):
        slot = turn(layer, k)
        return remote(held.at[slot, h], far_in.at[slot, h], 1, slot, h, far)

    def back(layer, h):
        place = low.at[layer, h, mine]
        return remote(place, place, 2, layer, h, near)

    def reduce_middle(layer, h, k):
        to_near(layer, h).wait_recv()
        held[turn(layer, k), h] = (
            term[layer, h, mine].astype(jnp.float32) + near_in[layer, h].astype(jnp.float32)
        ).astype(jnp.bfloat16)
        to_far(layer, h, k).start()

    def reduce_last(layer, h, k):
        slot = turn(layer, k)
        to_far(layer, h, k).wait_recv()
        low[layer, h, mine] = (
            held[slot, h].astype(jnp.float32) + far_in[slot, h].astype(jnp.float32)
        ).astype(jnp.bfloat16)
        back(layer, h).start()

    def reduce_done(layer, h, k):
        back(layer, h).wait_recv()
        to_near(layer, h).wait_send()
        to_far(layer, h, k).wait_send()
        back(layer, h).wait_send()

    def project(layer, h, state):
        term[layer, h] = jnp.dot(
            state[h], down[layer], preferred_element_type=jnp.float32
        ).astype(jnp.bfloat16)
        to_near(layer, h).start()

    def enter(k, h):
        for j in range(emb_local // GROUP):
            x = received[k, h * sources : (h + 1) * sources, :, j * GROUP : (j + 1) * GROUP]
            emb[k % 2, h, :, j * cols : (j + 1) * cols] = lax.dot_general(
                x.reshape(cols, part),
                placing[...],
                (((0,), (0,)), ((), ())),
                preferred_element_type=jnp.float32,
            ).astype(jnp.bfloat16)
        project(0, h, emb.at[k % 2])

    tile = width // TILES

    def cross(layer, h, first, state, store):
        for n in range(TILES):
            at = slice(n * tile, (n + 1) * tile)
            high = (
                jnp.dot(low[layer, h], up[layer, :, at], preferred_element_type=jnp.float32)
                + bias_ref[layer, at][None, :]
            )
            store(
                at,
                (
                    first[h, :, at].astype(jnp.float32) * high
                    + state[h, :, at].astype(jnp.float32)
                ).astype(jnp.bfloat16),
            )

    def out_copy(k, h):
        span = pl.ds(pl.multiple_of((h * chunks + k) * part, part), part)
        return pltpu.make_async_copy(result.at[h], out_ref.at[span], out_sem.at[h])

    def leave(k):
        for h in range(2):
            reduce_last(1, h, k)
        for h in range(2):
            reduce_done(1, h, k)

            @pl.when(k > 0)
            def _(h=h):
                out_copy(k - 1, h).wait()

            def to_out(at, value, h=h):
                result[h, :, at] = value

            cross(1, h, emb.at[k % 2], mid, to_out)
            out_copy(k, h).start()

    @pl.loop(0, chunks)
    def _(k):
        ahead = k + AHEAD
        more = ahead < chunks

        def look_up(phase):
            for p in range(pairs):
                if p * PHASES // pairs == phase:

                    @pl.when(more)
                    def _(p=p):
                        gather(ahead, p)

        @pl.when(more)
        def _():
            ids_wait(ahead)

            @pl.when(ahead >= ring)
            def _():
                exchanged(ahead - ring).wait_send()

        exchanged(k).wait_recv()
        for h in range(2):
            enter(k, h)
        look_up(0)
        for h in range(2):
            reduce_middle(0, h, k)

        @pl.when(k > 0)
        def _():
            leave(k - 1)

        look_up(1)
        look_up(2)
        for h in range(2):
            reduce_last(0, h, k)
        for h in range(2):
            reduce_done(0, h, k)

            def to_mid(at, value, h=h):
                mid[h, :, at] = value

            cross(0, h, emb.at[k % 2], emb.at[k % 2], to_mid)
            project(1, h, mid)
        look_up(3)

        @pl.when(more)
        def _():
            send(ahead, pl.ds(0, slots))
            keep(ahead)

        for h in range(2):
            reduce_middle(1, h, k)

    leave(chunks - 1)
    for h in range(2):
        out_copy(chunks - 1, h).wait()

    @pl.loop(max(chunks - ring, 0), chunks)
    def _(k):
        exchanged(k).wait_send()


def pipeline(table_feature, bias, ids, tables, cross_down, cross_up, sources, groups):
    slots, buckets, emb_dim = tables.shape
    layers, width, rank = cross_down.shape
    feats = table_feature.shape[0]
    emb_local = emb_dim // groups
    part = LANES
    share = part // 2
    chunks = ids.shape[1] // sources // (2 * part)
    pairs = slots // 2
    blocks = CORES * sources
    dma = pltpu.SemaphoreType.DMA
    bf16, f32 = jnp.bfloat16, jnp.float32
    return pl.pallas_call(
        functools.partial(kernel, sources, groups),
        out_shape=jax.ShapeDtypeStruct((chunks * 2 * part, width), bf16),
        in_specs=[
            pl.BlockSpec(memory_space=pltpu.SMEM),
            pl.BlockSpec(memory_space=pltpu.VMEM),
        ]
        + [pl.BlockSpec(memory_space=pl.ANY)] * 4,
        out_specs=pl.BlockSpec(memory_space=pl.ANY),
        scratch_shapes=[
            pltpu.SMEM((chunks, sources, slots, part), jnp.int32),
            pltpu.VMEM((2, 2, buckets // STEPS, emb_dim), bf16),
            pltpu.VMEM((pairs * buckets, emb_dim), f32),
            pltpu.VMEM((sources * part, emb_dim), f32),
            pltpu.VMEM((min(AHEAD + 1, chunks), blocks, slots, emb_local, part), bf16),
            pltpu.VMEM((chunks, blocks, slots, emb_local, part), bf16),
            pltpu.VMEM((layers, width, rank), bf16),
            pltpu.VMEM((layers, rank, width), bf16),
            pltpu.VMEM((feats * GROUP, feats * GROUP), bf16),
            pltpu.VMEM((2, 2, part, width), bf16),
            pltpu.VMEM((2, part, width), bf16),
            pltpu.VMEM((2, part, width), bf16),
            pltpu.VMEM((layers, 2, part, rank), bf16),
            pltpu.VMEM((layers, 2, share, rank), bf16),
            pltpu.VMEM((2 * layers, 2, share, rank), bf16),
            pltpu.VMEM((2 * layers, 2, share, rank), bf16),
            pltpu.VMEM((layers, 2, part, rank), bf16),
            dma((chunks,)),
            dma((2,)),
            dma((2,)),
            dma((chunks,)),
            dma((chunks,)),
            dma((3, 2 * layers, 2)),
            dma((3, 2 * layers, 2)),
            dma((2,)),
        ],
        compiler_params=pltpu.CompilerParams(
            collective_id=0, has_side_effects=True, vmem_limit_bytes=LIMIT
        ),
        name="pipeline",
    )(table_feature, bias, ids, tables, cross_down, cross_up)


def finish_kernel(x_ref, out_ref, held, read_sem, write_sem):
    pieces, rows = held.shape[:2]

    def read(i):
        return pltpu.make_async_copy(x_ref.at[pl.ds(i * rows, rows)], held.at[i], read_sem.at[i])

    def write(i):
        return pltpu.make_async_copy(held.at[i], out_ref.at[pl.ds(i * rows, rows)], write_sem.at[i])

    for i in range(pieces):
        read(i).start()
    for i in range(pieces):
        read(i).wait()
        write(i).start()
    for i in range(pieces):
        write(i).wait()


def finish(x):
    rows, width = x.shape
    dma = pltpu.SemaphoreType.DMA
    return pl.pallas_call(
        finish_kernel,
        out_shape=jax.ShapeDtypeStruct(x.shape, x.dtype),
        in_specs=[pl.BlockSpec(memory_space=pl.ANY)],
        out_specs=pl.BlockSpec(memory_space=pl.ANY),
        scratch_shapes=[
            pltpu.VMEM((PIECES, rows // PIECES, width), x.dtype),
            dma((PIECES,)),
            dma((PIECES,)),
        ],
        compiler_params=pltpu.CompilerParams(vmem_limit_bytes=LIMIT),
        name="finish",
    )(x)


def per_device(lookup_ids, table_feature, tables, cross_down, cross_up, cross_bias):
    sources = lax.axis_size("batch")
    groups = lax.axis_size("mp")
    return finish(
        pipeline(
            table_feature, cross_bias, lookup_ids, tables, cross_down, cross_up, sources, groups
        )
    )


def solution(mesh):
    return jax.shard_map(
        per_device,
        mesh=mesh,
        in_specs=(
            P("batch", None),
            P(),
            P("batch", None, None),
            P(None, "mp", None),
            P(None, None, "mp"),
            P(None, "mp"),
        ),
        out_specs=P("batch", "mp"),
        check_vma=False,
    )
```

```python
import functools

import jax
import jax.numpy as jnp
from jax import lax
from jax.experimental import pallas as pl
from jax.experimental.pallas import tpu as pltpu
from jax.sharding import PartitionSpec as P

MESH = pl.DeviceIdType.MESH
GROUP = 16
LANES = 128
CORES = 2
TILES = 4
AHEAD = 3
PHASES = 4
STEPS = 4
PIECES = 8
LIMIT = 67_043_328


def partner(me, mask, size):
    other = me
    bit = 1
    while bit < size:
        if mask & bit:
            other = other + bit * (1 - 2 * ((me // bit) % 2))
        bit *= 2
    return other


def kernel(
    sources,
    groups,
    feature_ref,
    bias_ref,
    ids_ref,
    tables_ref,
    down_ref,
    up_ref,
    out_ref,
    ids,
    stage,
    wide,
    rows,
    sent,
    received,
    down,
    up,
    placing,
    emb,
    mid,
    result,
    term,
    near_in,
    held,
    far_in,
    low,
    ids_sem,
    stage_sem,
    weight_sem,
    send_sem,
    recv_sem,
    reduce_send,
    reduce_recv,
    out_sem,
):
    b, m = lax.axis_index("batch"), lax.axis_index("mp")
    core = m % CORES
    side = m // CORES
    chunks, blocks, slots, emb_local, part = received.shape
    ring = sent.shape[0]
    pairs = slots // 2
    buckets = tables_ref.shape[1]
    emb_dim = tables_ref.shape[2]
    shared = emb_dim // 2
    width = down.shape[1]
    cols = placing.shape[0]
    feats = feature_ref.shape[0]
    near = (b, partner(m, 1, groups))
    far = (b, partner(m, CORES, groups))
    peers = [
        (partner(b, x, sources), side * CORES + partner(core, y, CORES), partner(core, y, CORES))
        for x in range(sources - 1, -1, -1)
        for y in range(CORES - 1, -1, -1)
        if (x, y) != (0, 0)
    ]

    def ids_copy(k, d):
        start = d * (2 * chunks * part) + (core * chunks + k) * part
        return pltpu.make_async_copy(
            ids_ref.at[:, pl.ds(pl.multiple_of(start, part), part)], ids.at[k, d], ids_sem.at[k]
        )

    span = buckets // STEPS

    def stage_copy(i):
        return pltpu.make_async_copy(
            tables_ref.at[pl.ds(2 * (i // STEPS), 2), pl.ds(i % STEPS * span, span)],
            stage.at[i % 2],
            stage_sem.at[i % 2],
        )

    stage_copy(0).start()
    for d in range(sources):
        ids_copy(0, d).start()
    stage_copy(1).start()

    barrier = pltpu.get_barrier_semaphore()
    greeted = [(x, y) for x, y, _ in peers] + [far]
    for peer in greeted:
        pl.semaphore_signal(barrier, inc=1, device_id=peer, device_id_type=MESH)

    @pl.loop(1, chunks)
    def _(k):
        for d in range(sources):
            ids_copy(k, d).start()

    weights = [
        pltpu.make_async_copy(down_ref, down, weight_sem.at[0]),
        pltpu.make_async_copy(up_ref, up, weight_sem.at[1]),
    ]

    def convert(p):
        for i in range(p * STEPS, (p + 1) * STEPS):
            stage_copy(i).wait()
            step = min(1024, span)

            @pl.loop(0, span // step)
            def _(t, i=i):
                at = pl.ds(pl.multiple_of(t * step, step), step)
                to = pl.ds(pl.multiple_of(i * span + t * step, step), step)
                lane = lax.broadcasted_iota(jnp.int32, (step, emb_dim), 1)
                own = stage[i % 2, side, at, :].astype(jnp.float32)
                other = pltpu.roll(stage[i % 2, 1 - side, at, :].astype(jnp.float32), shared, 1)
                wide[to, :] = jnp.where(lane // shared == side, own, other)

            if i + 2 < pairs * STEPS:
                stage_copy(i + 2).start()

    def gather(k, p):
        lower = lax.broadcasted_iota(jnp.int32, (1, emb_dim), 1) < shared
        table = wide.at[pl.ds(p * buckets, buckets)]

        @pl.loop(0, sources)
        def _(d):
            base = pl.multiple_of(d * part, part)
            for u in range(part):
                one = table[pl.ds(ids[k, d, 2 * p, u], 1), :]
                two = table[pl.ds(ids[k, d, 2 * p + 1, u], 1), :]
                rows[pl.ds(base + u, 1), :] = jnp.where(lower, one, two)

        for d in range(sources):
            turned = rows[d * part : (d + 1) * part, :].T.astype(jnp.bfloat16)
            for s in range(2):
                for c in range(CORES):
                    at = s * shared + c * emb_local
                    sent[k % ring, d * CORES + c, 2 * p + s] = turned[at : at + emb_local]

    def send(k, span):
        for x, y, c in peers:
            pltpu.make_async_remote_copy(
                src_ref=sent.at[k % ring, x * CORES + c, span],
                dst_ref=received.at[k, core * sources + b, span],
                send_sem=send_sem.at[k],
                recv_sem=recv_sem.at[k],
                device_id=(x, y),
                device_id_type=MESH,
            ).start()

    def keep(k):
        received[k, core * sources + b] = sent[k % ring, b * CORES + core]

    def exchanged(k):
        span = pl.ds(0, blocks - 1)
        return pltpu.make_async_remote_copy(
            src_ref=sent.at[k % ring, span],
            dst_ref=received.at[k, span],
            send_sem=send_sem.at[k],
            recv_sem=recv_sem.at[k],
            device_id=near,
            device_id_type=MESH,
        )

    def ids_wait(k):
        pltpu.make_async_copy(ids.at[k], ids.at[k], ids_sem.at[k]).wait()

    ids_wait(0)
    for p in range(pairs):
        convert(p)
        gather(0, p)
        if p == 0:
            pl.semaphore_wait(barrier, len(greeted))
        send(0, pl.ds(2 * p, 2))
    keep(0)
    for copy in weights:
        copy.start()

    @pl.loop(1, min(AHEAD, chunks))
    def _(k):
        ids_wait(k)
        for p in range(pairs):
            gather(k, p)
        send(k, pl.ds(0, slots))
        keep(k)

    @pl.loop(0, feats)
    def _(s):
        column = lax.broadcasted_iota(jnp.int32, (GROUP, cols), 1)
        e = lax.broadcasted_iota(jnp.int32, (GROUP, cols), 0)
        placing[pl.ds(pl.multiple_of(s * GROUP, GROUP), GROUP), :] = jnp.where(
            column == feature_ref[s] + feats * e, 1.0, 0.0
        ).astype(jnp.bfloat16)

    for copy in weights:
        copy.wait()

    share = part // 2
    mine = pl.ds(pl.multiple_of(core * share, share), share)
    theirs = pl.ds(pl.multiple_of((1 - core) * share, share), share)

    def remote(src, dst, kind, layer, h, peer):
        return pltpu.make_async_remote_copy(
            src_ref=src,
            dst_ref=dst,
            send_sem=reduce_send.at[kind, layer, h],
            recv_sem=reduce_recv.at[kind, layer, h],
            device_id=peer,
            device_id_type=MESH,
        )

    def to_near(layer, h):
        return remote(term.at[layer, h, theirs], near_in.at[layer, h], 0, layer, h, near)

    def turn(layer, k):
        return 2 * layer + k % 2

    def to_far(layer, h, k):
        slot = turn(layer, k)
        return remote(held.at[slot, h], far_in.at[slot, h], 1, slot, h, far)

    def back(layer, h):
        place = low.at[layer, h, mine]
        return remote(place, place, 2, layer, h, near)

    def reduce_middle(layer, h, k):
        to_near(layer, h).wait_recv()
        held[turn(layer, k), h] = (
            term[layer, h, mine].astype(jnp.float32) + near_in[layer, h].astype(jnp.float32)
        ).astype(jnp.bfloat16)
        to_far(layer, h, k).start()

    def reduce_last(layer, h, k):
        slot = turn(layer, k)
        to_far(layer, h, k).wait_recv()
        low[layer, h, mine] = (
            held[slot, h].astype(jnp.float32) + far_in[slot, h].astype(jnp.float32)
        ).astype(jnp.bfloat16)
        back(layer, h).start()

    def reduce_done(layer, h, k):
        back(layer, h).wait_recv()
        to_near(layer, h).wait_send()
        to_far(layer, h, k).wait_send()
        back(layer, h).wait_send()

    def project(layer, h, state):
        term[layer, h] = jnp.dot(
            state[h], down[layer], preferred_element_type=jnp.float32
        ).astype(jnp.bfloat16)
        to_near(layer, h).start()

    def enter(k):
        first = emb.at[k % 2]
        for j in range(emb_local // GROUP):
            at = slice(j * cols, (j + 1) * cols)
            sides = [
                received[
                    k, h * sources : (h + 1) * sources, :, j * GROUP : (j + 1) * GROUP
                ].reshape(cols, part)
                for h in range(2)
            ]
            placed = lax.dot_general(
                jnp.concatenate(sides, axis=1),
                placing[...],
                (((0,), (0,)), ((), ())),
                preferred_element_type=jnp.float32,
            ).astype(jnp.bfloat16)
            for h in range(2):
                first[h, :, at] = placed[h * part : (h + 1) * part]
        low_part = jnp.dot(
            first[...].reshape(2 * part, width), down[0], preferred_element_type=jnp.float32
        ).astype(jnp.bfloat16)
        for h in range(2):
            term[0, h] = low_part[h * part : (h + 1) * part]
            to_near(0, h).start()

    tile = width // TILES

    def cross(layer, h, first, state, store):
        for n in range(TILES):
            at = slice(n * tile, (n + 1) * tile)
            high = (
                jnp.dot(low[layer, h], up[layer, :, at], preferred_element_type=jnp.float32)
                + bias_ref[layer, at][None, :]
            )
            store(
                at,
                (
                    first[h, :, at].astype(jnp.float32) * high
                    + state[h, :, at].astype(jnp.float32)
                ).astype(jnp.bfloat16),
            )

    def out_copy(k, h):
        span = pl.ds(pl.multiple_of((h * chunks + k) * part, part), part)
        return pltpu.make_async_copy(result.at[h], out_ref.at[span], out_sem.at[h])

    def leave(k):
        for h in range(2):
            reduce_last(1, h, k)
        for h in range(2):
            reduce_done(1, h, k)

            @pl.when(k > 0)
            def _(h=h):
                out_copy(k - 1, h).wait()

            def to_out(at, value, h=h):
                result[h, :, at] = value

            cross(1, h, emb.at[k % 2], mid, to_out)
            out_copy(k, h).start()

    @pl.loop(0, chunks)
    def _(k):
        ahead = k + AHEAD
        more = ahead < chunks

        def look_up(phase):
            for p in range(pairs):
                if p * PHASES // pairs == phase:

                    @pl.when(more)
                    def _(p=p):
                        gather(ahead, p)

        @pl.when(more)
        def _():
            ids_wait(ahead)

            @pl.when(ahead >= ring)
            def _():
                exchanged(ahead - ring).wait_send()

        exchanged(k).wait_recv()
        enter(k)
        look_up(0)
        for h in range(2):
            reduce_middle(0, h, k)

        @pl.when(k > 0)
        def _():
            leave(k - 1)

        look_up(1)
        look_up(2)
        for h in range(2):
            reduce_last(0, h, k)
        for h in range(2):
            reduce_done(0, h, k)

            def to_mid(at, value, h=h):
                mid[h, :, at] = value

            cross(0, h, emb.at[k % 2], emb.at[k % 2], to_mid)
            project(1, h, mid)
        look_up(3)

        @pl.when(more)
        def _():
            send(ahead, pl.ds(0, slots))
            keep(ahead)

        for h in range(2):
            reduce_middle(1, h, k)

    leave(chunks - 1)
    for h in range(2):
        out_copy(chunks - 1, h).wait()

    @pl.loop(max(chunks - ring, 0), chunks)
    def _(k):
        exchanged(k).wait_send()


def pipeline(table_feature, bias, ids, tables, cross_down, cross_up, sources, groups):
    slots, buckets, emb_dim = tables.shape
    layers, width, rank = cross_down.shape
    feats = table_feature.shape[0]
    emb_local = emb_dim // groups
    part = LANES
    share = part // 2
    chunks = ids.shape[1] // sources // (2 * part)
    pairs = slots // 2
    blocks = CORES * sources
    dma = pltpu.SemaphoreType.DMA
    bf16, f32 = jnp.bfloat16, jnp.float32
    return pl.pallas_call(
        functools.partial(kernel, sources, groups),
        out_shape=jax.ShapeDtypeStruct((chunks * 2 * part, width), bf16),
        in_specs=[
            pl.BlockSpec(memory_space=pltpu.SMEM),
            pl.BlockSpec(memory_space=pltpu.VMEM),
        ]
        + [pl.BlockSpec(memory_space=pl.ANY)] * 4,
        out_specs=pl.BlockSpec(memory_space=pl.ANY),
        scratch_shapes=[
            pltpu.SMEM((chunks, sources, slots, part), jnp.int32),
            pltpu.VMEM((2, 2, buckets // STEPS, emb_dim), bf16),
            pltpu.VMEM((pairs * buckets, emb_dim), f32),
            pltpu.VMEM((sources * part, emb_dim), f32),
            pltpu.VMEM((min(AHEAD + 1, chunks), blocks, slots, emb_local, part), bf16),
            pltpu.VMEM((chunks, blocks, slots, emb_local, part), bf16),
            pltpu.VMEM((layers, width, rank), bf16),
            pltpu.VMEM((layers, rank, width), bf16),
            pltpu.VMEM((feats * GROUP, feats * GROUP), bf16),
            pltpu.VMEM((2, 2, part, width), bf16),
            pltpu.VMEM((2, part, width), bf16),
            pltpu.VMEM((2, part, width), bf16),
            pltpu.VMEM((layers, 2, part, rank), bf16),
            pltpu.VMEM((layers, 2, share, rank), bf16),
            pltpu.VMEM((2 * layers, 2, share, rank), bf16),
            pltpu.VMEM((2 * layers, 2, share, rank), bf16),
            pltpu.VMEM((layers, 2, part, rank), bf16),
            dma((chunks,)),
            dma((2,)),
            dma((2,)),
            dma((chunks,)),
            dma((chunks,)),
            dma((3, 2 * layers, 2)),
            dma((3, 2 * layers, 2)),
            dma((2,)),
        ],
        compiler_params=pltpu.CompilerParams(
            collective_id=0, has_side_effects=True, vmem_limit_bytes=LIMIT
        ),
        name="pipeline",
    )(table_feature, bias, ids, tables, cross_down, cross_up)


def finish_kernel(x_ref, out_ref, held, read_sem, write_sem):
    pieces, rows = held.shape[:2]

    def read(i):
        return pltpu.make_async_copy(x_ref.at[pl.ds(i * rows, rows)], held.at[i], read_sem.at[i])

    def write(i):
        return pltpu.make_async_copy(held.at[i], out_ref.at[pl.ds(i * rows, rows)], write_sem.at[i])

    for i in range(pieces):
        read(i).start()
    for i in range(pieces):
        read(i).wait()
        write(i).start()
    for i in range(pieces):
        write(i).wait()


def finish(x):
    rows, width = x.shape
    dma = pltpu.SemaphoreType.DMA
    return pl.pallas_call(
        finish_kernel,
        out_shape=jax.ShapeDtypeStruct(x.shape, x.dtype),
        in_specs=[pl.BlockSpec(memory_space=pl.ANY)],
        out_specs=pl.BlockSpec(memory_space=pl.ANY),
        scratch_shapes=[
            pltpu.VMEM((PIECES, rows // PIECES, width), x.dtype),
            dma((PIECES,)),
            dma((PIECES,)),
        ],
        compiler_params=pltpu.CompilerParams(vmem_limit_bytes=LIMIT),
        name="finish",
    )(x)


def per_device(lookup_ids, table_feature, tables, cross_down, cross_up, cross_bias):
    sources = lax.axis_size("batch")
    groups = lax.axis_size("mp")
    return finish(
        pipeline(
            table_feature, cross_bias, lookup_ids, tables, cross_down, cross_up, sources, groups
        )
    )


def solution(mesh):
    return jax.shard_map(
        per_device,
        mesh=mesh,
        in_specs=(
            P("batch", None),
            P(),
            P("batch", None, None),
            P(None, "mp", None),
            P(None, None, "mp"),
            P(None, "mp"),
        ),
        out_specs=P("batch", "mp"),
        check_vma=False,
    )
```
